256 devices in a mesh: lat: 32 (over y_hi, z, core), lon: 8 (over y_lo, x).
Axes of the slice: x: 4, y: 4 (y_hi: 2, y_lo: 2; y = y_hi * 2 + y_lo), z: 8, core: 2. Of those that a mesh axis runs over, the one named last changes fastest.
Arguments:
- features: bfloat16 [512, 512, 512], P('lat', 'lon'), may hold values from -6 to 6
- upstream: bfloat16 [512, 512, 512], P('lat', 'lon'), may hold values from -6 to 6
- kernel: bfloat16 [4608, 512], replicated, may hold values from -0.09375 to 0.09375
Outputs:
- input_grad: bfloat16 [512, 512, 512], P('lat', 'lon')
- direction: float32 [4608, 512], P('lat')
- perturbed: float32 [4608, 512], P('lat')
The draws below stay inside these ranges and needn't reach their ends.
All inputs are finite; a program needn't handle non-finite values.
Results may differ from the reference program's by a relative error of at most 0.0032.
Values may be sent and summed in bfloat16 or wider, within the bound.
A program may use at most 128 MiB of HBM per device.

```python
import jax
import jax.numpy as jnp
from jax import lax

C = 512
NLAT = 512
NLON = 512


def block_levels(stream_key, extent, pieces, low, top_value):
    level, own = 1.0, jax.random.fold_in(stream_key, 6)
    for dim, blocks in pieces:
        draws = jnp.exp(jax.random.uniform(jax.random.fold_in(own, dim), (blocks,), jnp.float32, low / len(pieces), top_value / len(pieces)))
        level = level * jnp.repeat(draws, extent[dim] // blocks).reshape([-1 if axis == dim else 1 for axis in range(len(extent))])
    return level


def centred(key, dims, spread, most, split=(), held_as=jnp.bfloat16):
    entries = spread * jax.random.normal(key, dims, jnp.float32)
    if split:
        entries = entries * block_levels(key, dims, split, -0.22, 0.18)
    return jnp.clip(entries, -most, most).astype(held_as)


def setup_inputs(seed: int = 0) -> dict:
    arg_keys = jax.random.split(jax.random.key(seed), 4)
    return {
        "features": centred(arg_keys[0], (NLAT, NLON, C), 1.0, 6.0, ((0, 32), (1, 8))),
        "upstream": centred(arg_keys[1], (NLAT, NLON, C), 1.0, 6.0, ((0, 32), (1, 8))),
        "kernel": centred(arg_keys[2], (9 * C, C), (9 * C) ** -0.5, 0.09375),
    }


def extend(field):
    wrapped = jnp.concatenate([field[:, -1:], field, field[:, :1]], axis=1)
    return jnp.pad(wrapped, ((1, 1), (0, 0), (0, 0)))

def reference(features, upstream, kernel):
    height, breadth, channels = features.shape
    padded_x = extend(features)
    z = jnp.zeros((height, breadth, channels), jnp.float32)
    for a in range(3):
        for b in range(3):
            t = 3 * a + b
            z = z + jnp.dot(padded_x[a:a + height, b:b + breadth], kernel[t * channels:(t + 1) * channels], preferred_element_type=jnp.float32)
    sig = jax.nn.sigmoid(z)
    slope = (upstream.astype(jnp.float32) * sig * (1.0 + z * (1.0 - sig))).astype(jnp.bfloat16)
    padded_slope = extend(slope)
    back = upstream.astype(jnp.float32)
    blocks = []
    for a in range(3):
        for b in range(3):
            t = 3 * a + b
            piece = padded_slope[2 - a:2 - a + height, 2 - b:2 - b + breadth]
            back = back + lax.dot_general(piece, kernel[t * channels:(t + 1) * channels], (((2,), (1,)), ((), ())), preferred_element_type=jnp.float32)
            blocks.append(lax.dot_general(padded_x[a:a + height, b:b + breadth], slope, (((0, 1), (0, 1)), ((), ())), preferred_element_type=jnp.float32))
    input_grad = back.astype(jnp.bfloat16)
    grad = jnp.concatenate(blocks, axis=0)
    count = 9.0 * channels * channels
    total = jnp.sum(grad * grad)
    direction = grad / jnp.sqrt(total / count + 1e-06)
    perturbed = kernel.astype(jnp.float32) + 0.05 / jnp.sqrt(count) * direction
    return (input_grad, direction, perturbed)
```

```python
import functools

import jax
import jax.numpy as jnp
from jax import lax
from jax.experimental import pallas as pl
from jax.experimental.pallas import tpu as pltpu
from jax.sharding import PartitionSpec as P

MESH = pl.DeviceIdType.MESH
F32, BF16 = jnp.float32, jnp.bfloat16

H, W, C = 16, 64, 512
POS = H * W
YHI, ZN, LON, LAT = 2, 8, 8, 32
PR, PC = 72, 128
BLOCK = 144

ORDERS = (
    (("x", "A"), ("x", "B"), ("y", "A"), ("y", "B")),
    (("y", "A"), ("y", "B"), ("x", "A"), ("x", "B")),
    (("x", "B"), ("x", "A"), ("y", "B"), ("y", "A")),
    (("y", "B"), ("y", "A"), ("x", "B"), ("x", "A")),
)
GROUPS = (
    (((0, 0), (0, 384), (0, 768)), ((1, 768), (1, 1152), (2, 0))),
    (((0, 1152), (1, 0), (1, 384)), ((2, 384), (2, 768), (2, 1152))),
)


def flip(p):
    return p + 1 - 2 * (p % 2)


def gated(upstream, z):
    sig = jax.nn.sigmoid(z)
    return upstream.astype(F32) * sig * (1.0 + z * (1.0 - sig))


def kernel(
    x_hbm, u_hbm, k_hbm, ig_hbm, dir_hbm, per_hbm,
    x_v, u_v, k_v, x3, s3, s_v, ig_v, dir_v, per_v,
    colx, hrowx, hcolx, hcorx, cols, hrows, hcols, hcors,
    acc, csend, crecv, send1, send2, send3, send4, recv1, recv2, recv3, recv4,
    pieces, zsend, zrecv, ag, norms,
    lsem, hsx, hrx, hss, hrs, cs_sem, cr_sem, ss_sem, sr_sem, zs_sem, zr_sem, as_sem, ar_sem, ns_sem, nr_sem,
):
    lat, lon = lax.axis_index("lat"), lax.axis_index("lon")
    core, zc, yhi = lat % 2, (lat // 2) % 8, lat // 16
    xc, ylo = lon % 4, lon // 4
    yc = 2 * yhi + ylo

    def place(yy, zz, cc, xx):
        return ((yy // 2) * 16 + zz * 2 + cc, (yy % 2) * 4 + xx)

    def x_peer(q):
        return place(yc, zc, core, q)

    def y_peer(q):
        return place(q, zc, core, xc)

    def z_peer(q):
        return place(yc, q, core, xc)

    up, down = (lat + LAT - 1) % LAT, (lat + 1) % LAT
    left, right = (lon + LON - 1) % LON, (lon + 1) % LON

    loads = [
        pltpu.make_async_copy(src, dst, lsem.at[i])
        for i, (src, dst) in enumerate(((x_hbm, x_v), (k_hbm, k_v), (u_hbm, u_v)))
    ]
    for load in loads:
        load.start()

    barrier = pltpu.get_barrier_semaphore()
    greeted = [
        (up, lon), (down, lon), (lat, left), (lat, right),
        (up, left), (up, right), (down, left), (down, right),
        x_peer(flip(xc)), x_peer(3 - xc), y_peer(flip(yc)), y_peer(3 - yc),
    ] + [z_peer((zc + d) % ZN) for d in range(1, ZN)]
    for peer in greeted:
        pl.semaphore_signal(barrier, inc=1, device_id=peer, device_id_type=MESH)

    def remote(src, dst, ssem, rsem, peer):
        return pltpu.make_async_remote_copy(
            src_ref=src, dst_ref=dst, send_sem=ssem, recv_sem=rsem, device_id=peer, device_id_type=MESH
        )

    def edge_columns(src, col):
        def body(h, carry):
            base = pl.multiple_of(h * W, W)
            col[0, pl.ds(h, 1), :] = src[pl.ds(base, 16), :].astype(F32)[0:1]
            col[1, pl.ds(h, 1), :] = src[pl.ds(base + W - 16, 16), :].astype(F32)[15:16]
            return carry
        lax.fori_loop(0, H, body, 0)

    def halo(src, col, hrow, hcol, hcor, ssem, rsem):
        plan = (
            (src.at[pl.ds((H - 1) * W, W)], hrow.at[0], (down, lon)),
            (src.at[pl.ds(0, W)], hrow.at[1], (up, lon)),
            (col.at[1], hcol.at[0], (lat, right)),
            (col.at[0], hcol.at[1], (lat, left)),
            (col.at[1, pl.ds(8, 8)], hcor.at[0], (down, right)),
            (col.at[0, pl.ds(8, 8)], hcor.at[1], (down, left)),
            (col.at[1, pl.ds(0, 8)], hcor.at[2], (up, right)),
            (col.at[0, pl.ds(0, 8)], hcor.at[3], (up, left)),
        )
        return [remote(a, b, ssem.at[i], rsem.at[i], peer) for i, (a, b, peer) in enumerate(plan)]

    rows = lax.broadcasted_iota(jnp.int32, (W, C), 0)
    above = jnp.where(lat == 0, 0.0, 1.0).astype(F32)
    below = jnp.where(lat == LAT - 1, 0.0, 1.0).astype(F32)

    def shifted(dst, base, row, low, high):
        dst[pl.ds(base, W), C : 2 * C] = row.astype(BF16)
        dst[pl.ds(base, W), 0:C] = jnp.where(rows == 0, low, pltpu.roll(row, 1, 0)).astype(BF16)
        dst[pl.ds(base, W), 2 * C : 3 * C] = jnp.where(rows == W - 1, high, pltpu.roll(row, W - 1, 0)).astype(BF16)

    def build(src, hrow, hcol, hcor, dst):
        def body(h, carry):
            base = pl.multiple_of(h * W, W)
            shifted(
                dst, pl.multiple_of(base + W, W), src[pl.ds(base, W), :].astype(F32),
                hcol[0, pl.ds(h, 1), :], hcol[1, pl.ds(h, 1), :],
            )
            return carry
        lax.fori_loop(0, H, body, 0)
        shifted(dst, 0, hrow[0].astype(F32) * above, hcor[0, 7:8, :] * above, hcor[1, 7:8, :] * above)
        shifted(
            dst, (H + 1) * W, hrow[1].astype(F32) * below, hcor[2, 0:1, :] * below, hcor[3, 0:1, :] * below
        )

    loads[0].wait()
    edge_columns(x_v, colx)
    pl.semaphore_wait(barrier, len(greeted))
    halo_x = halo(x_v, colx, hrowx, hcolx, hcorx, hsx, hrx)
    for copy in halo_x:
        copy.start()
    loads[1].wait()
    loads[2].wait()
    for copy in halo_x:
        copy.wait_recv()
    build(x_v, hrowx, hcolx, hcorx, x3)

    for c in range(4):
        z = jnp.zeros((256, C), F32)
        for a in range(3):
            z = z + jnp.dot(
                x3[(4 * c + a) * W : (4 * c + a) * W + 256, :],
                k_v[a * 3 * C : (a + 1) * 3 * C, :],
                preferred_element_type=F32,
            )
        s_v[256 * c : 256 * (c + 1), :] = gated(u_v[256 * c : 256 * (c + 1), :], z).astype(BF16)

    edge_columns(s_v, cols)
    halo_s = halo(s_v, cols, hrows, hcols, hcors, hss, hrs)
    for copy in halo_s:
        copy.start()

    partner = (flip(lat), lon)
    core_copies = [
        remote(csend.at[u], crecv.at[u], cs_sem.at[u], cr_sem.at[u], partner) for u in range(8)
    ]

    def weight_group(j):
        for hi in range(2):
            for m, (a, first) in enumerate(GROUPS[j][hi]):
                part = lax.dot_general(
                    x3[a * W : a * W + POS, first : first + 384],
                    s_v[...],
                    (((0,), (0,)), ((), ())),
                    preferred_element_type=F32,
                )
                row = 384 * m
                while row < 384 * (m + 1):
                    stop = min(384 * (m + 1), (row // PR + 1) * PR)
                    p = row // PR
                    zl, cc, lo = p // 4, (p // 2) % 2, p % 2
                    for xt in range(4):
                        acc[cc, 4 * j + zl, 2 * hi + lo, xt, row % PR : row % PR + stop - row, :] = part[
                            row - 384 * m : stop - 384 * m, PC * xt : PC * (xt + 1)
                        ]
                    row = stop
        for zl in range(4):
            u = 4 * j + zl
            for yy in range(4):
                for xx in range(4):
                    csend[u, 4 * yy + xx] = acc[1 - core, u, yy, xx].astype(BF16)
            core_copies[u].start()

    weight_group(0)
    weight_group(1)

    sends, recvs = (send1, send2, send3, send4), (recv1, recv2, recv3, recv4)

    def halves(kind, first, p):
        q = flip(p) if kind == "A" else 3 - p
        if first:
            other = (lambda c: 3 - c) if kind == "A" else flip
            return q, [(q, q), (other(q), other(q))], [(p, p), (other(p), other(p))]
        return q, [(q, 1)], [(p, 0)]

    started = {}

    def lists_after(u, steps):
        ys = [(i, i) for i in range(4)]
        xs = [(i, i) for i in range(4)]
        for s in range(steps):
            dim, kind = ORDERS[u % 4][s]
            _, _, keep = halves(kind, s % 2 == 0, xc if dim == "x" else yc)
            kept = [(v, i) for i, (v, _) in enumerate(keep)]
            if dim == "x":
                xs = kept
            else:
                ys = kept
        return ys, xs

    def advance(u, s):
        ys, xs = lists_after(u, s)
        if s == 0:
            core_copies[u].wait_recv()
            arrived = crecv
        else:
            started[u, s - 1].wait_recv()
            arrived = recvs[s - 1]
        wide = len(xs)
        dim, kind = ORDERS[u % 4][s]
        q, out, keep = halves(kind, s % 2 == 0, xc if dim == "x" else yc)
        send_y, send_x = (ys, out) if dim == "x" else (out, xs)
        keep_y, keep_x = (ys, keep) if dim == "x" else (keep, xs)
        slot = 0
        for yv, yi in send_y:
            for xv, xi in send_x:
                total = acc[core, u, yv, xv] + arrived[u, yi * wide + xi].astype(F32)
                sends[s][u, slot] = total.astype(BF16)
                slot += 1
        copy = remote(
            sends[s].at[u], recvs[s].at[u], ss_sem.at[s, u], sr_sem.at[s, u],
            x_peer(q) if dim == "x" else y_peer(q),
        )
        copy.start()
        started[u, s] = copy
        for yv, yi in keep_y:
            for xv, xi in keep_x:
                acc[core, u, yv, xv] = acc[core, u, yv, xv] + arrived[u, yi * wide + xi].astype(F32)

    def z_copy(u):
        return remote(zsend.at[u], zrecv.at[zc], zs_sem.at[u], zr_sem.at[zc], z_peer(u))

    def to_z(u):
        started[u, 3].wait_recv()
        total = acc[core, u, yc, xc] + recv4[u, 0].astype(F32)
        pieces[u] = total
        zsend[u] = total.astype(BF16)

        @pl.when(zc != u)
        def _():
            z_copy(u).start()

    def input_grad(c):
        n = 512
        total = u_v[n * c : n * (c + 1), :].astype(F32)
        grads = jnp.zeros((n, C), F32)
        for a in range(3):
            for b in range(3):
                t = 3 * a + b
                top = (8 * c + 2 - a) * W
                grads = grads + lax.dot_general(
                    s3[top : top + n, (2 - b) * C : (3 - b) * C],
                    k_v[t * C : (t + 1) * C, :],
                    (((1,), (1,)), ((), ())),
                    preferred_element_type=F32,
                )
        ig_v[n * c : n * (c + 1), :] = (total + grads).astype(BF16)

    first, second = range(4), range(4, 8)
    for u in first:
        advance(u, 0)
    for copy in halo_s:
        copy.wait_recv()
    build(s_v, hrows, hcols, hcors, s3)
    for u in second:
        advance(u, 0)
    input_grad(0)
    for u in first:
        advance(u, 1)
    input_grad(1)
    ig_copy = pltpu.make_async_copy(ig_v, ig_hbm, lsem.at[3])
    ig_copy.start()
    for u in second:
        advance(u, 1)
    for u in first:
        advance(u, 2)
    for u in second:
        advance(u, 2)
    for u in first:
        advance(u, 3)
    for u in second:
        advance(u, 3)
    for u in range(8):
        to_z(u)

    total = pieces[zc]
    for d in range(1, ZN):
        src = (zc + d) % ZN
        remote(zsend.at[0], zrecv.at[src], zs_sem.at[0], zr_sem.at[src], z_peer(src)).wait_recv()
        total = total + zrecv[src].astype(F32)

    ag[lon] = total
    ag_copies = []
    for d in range(1, LON):
        copy = remote(ag.at[lon], ag.at[lon], as_sem.at[d], ar_sem.at[lon], (lat, (lon + d) % LON))
        copy.start()
        ag_copies.append(copy)
    for d in range(1, LON):
        src = (lon + d) % LON
        remote(ag.at[src], ag.at[src], as_sem.at[0], ar_sem.at[src], (lat, src)).wait_recv()

    squares = jnp.zeros((PR, PC), F32)
    for i in range(LON):
        squares = squares + ag[i] * ag[i]
    norms[lat] = jnp.sum(squares, axis=0, keepdims=True)

    def norm_copy(d):
        return remote(
            norms.at[lat], norms.at[lat], ns_sem.at[d], nr_sem.at[lat], ((lat + d) % LAT, lon)
        )

    def norm_start(d, carry):
        norm_copy(d).start()
        return carry

    def norm_wait(d, carry):
        src = (lat + d) % LAT
        remote(norms.at[src], norms.at[src], ns_sem.at[d], nr_sem.at[src], (src, lon)).wait_recv()
        return carry

    lax.fori_loop(1, LAT, norm_start, 0)
    lax.fori_loop(1, LAT, norm_wait, 0)
    summed = jnp.sum(jnp.sum(norms[...], axis=0), axis=1, keepdims=True)
    count = 9.0 * C * C
    inverse = 1.0 / jnp.sqrt(summed / count + 1e-06)
    step = 0.05 / (count ** 0.5)
    own = k_v[pl.ds(pl.multiple_of(lat * BLOCK, 16), BLOCK), :].astype(F32)
    for i in range(LON):
        r0, c0 = (i // 4) * PR, (i % 4) * PC
        piece = ag[i] * inverse
        dir_v[r0 : r0 + PR, c0 : c0 + PC] = piece
        per_v[r0 : r0 + PR, c0 : c0 + PC] = own[r0 : r0 + PR, c0 : c0 + PC] + step * piece
    outs = [
        pltpu.make_async_copy(dir_v, dir_hbm, lsem.at[0]),
        pltpu.make_async_copy(per_v, per_hbm, lsem.at[1]),
    ]
    for copy in outs:
        copy.start()

    for copy in halo_x + halo_s + core_copies + list(started.values()) + ag_copies:
        copy.wait_send()
    for u in range(8):
        @pl.when(zc != u)
        def _():
            z_copy(u).wait_send()

    def norm_sent(d, carry):
        norm_copy(d).wait_send()
        return carry

    lax.fori_loop(1, LAT, norm_sent, 0)
    for copy in outs + [ig_copy]:
        copy.wait()


def shards(features, upstream, weights):
    any_spec = pl.BlockSpec(memory_space=pl.ANY)
    vmem = pltpu.VMEM
    dma = pltpu.SemaphoreType.DMA
    scratch = [
        vmem((POS, C), BF16), vmem((POS, C), BF16), vmem((9 * C, C), BF16),
        vmem(((H + 2) * W, 3 * C), BF16), vmem(((H + 2) * W, 3 * C), BF16), vmem((POS, C), BF16),
        vmem((POS, C), BF16), vmem((BLOCK, C), F32), vmem((BLOCK, C), F32),
    ]
    for _ in range(2):
        scratch += [vmem((2, H, C), F32), vmem((2, W, C), BF16), vmem((2, H, C), F32), vmem((4, 8, C), F32)]
    scratch += [vmem((2, 8, 4, 4, PR, PC), F32), vmem((8, 16, PR, PC), BF16), vmem((8, 16, PR, PC), BF16)]
    scratch += [vmem((8, n, PR, PC), BF16) for n in (8, 4, 2, 1)] * 2
    scratch += [
        vmem((8, PR, PC), F32), vmem((8, PR, PC), BF16), vmem((8, PR, PC), BF16),
        vmem((LON, PR, PC), F32), vmem((LAT, 1, PC), F32),
        dma((4,)), dma((8,)), dma((8,)), dma((8,)), dma((8,)), dma((8,)), dma((8,)),
        dma((4, 8)), dma((4, 8)), dma((8,)), dma((8,)), dma((8,)), dma((8,)), dma((LAT,)), dma((LAT,)),
    ]
    grad, direction, perturbed = pl.pallas_call(
        kernel,
        name="ascent",
        out_shape=(
            jax.ShapeDtypeStruct((POS, C), BF16),
            jax.ShapeDtypeStruct((BLOCK, C), F32),
            jax.ShapeDtypeStruct((BLOCK, C), F32),
        ),
        in_specs=[any_spec] * 3,
        out_specs=(any_spec,) * 3,
        scratch_shapes=scratch,
        compiler_params=pltpu.CompilerParams(
            collective_id=0, has_side_effects=True, vmem_limit_bytes=62 * 1024 * 1024
        ),
    )(features.reshape(POS, C), upstream.reshape(POS, C), weights)
    return grad.reshape(features.shape), direction, perturbed


def solution(mesh):
    return jax.shard_map(
        shards,
        mesh=mesh,
        in_specs=(P("lat", "lon", None), P("lat", "lon", None), P()),
        out_specs=(P("lat", "lon", None), P("lat", None), P("lat", None)),
        check_vma=False,
    )
```
